512 devices in a mesh: tau: 8 (over z_lo), row: 8 (over y, core), col: 8 (over x, z_hi).
Axes of the slice: x: 4, y: 4, z: 16 (z_hi: 2, z_lo: 8; z = z_hi * 8 + z_lo), core: 2. Of those that a mesh axis runs over, the one named last changes fastest.
Arguments:
- occupied: bfloat16 [8, 1024, 8192], P('tau', 'row', 'col'), may hold values from -6 to 6
- virtual_green: bfloat16 [8, 8192, 2048], P('tau', 'row', 'col'), may hold values from -0.0625 to 0.0625
- occ_mask: int32 [8, 64], P('row', 'col'), may hold values 0 or 1
- virt_mask: int32 [64, 16], P('row', 'col'), may hold values 0 or 1
- chi_mask: int32 [8, 16], P('row', 'col'), may hold values 0 or 1
- cosine_weights: float32 [8, 8], replicated, may hold values from -3 to 3
Outputs:
- chi_freq: float32 [8, 1024, 2048], P(None, ('row', 'tau'), 'col')
The draws below stay inside these ranges and needn't reach their ends.
All inputs are finite; a program needn't handle non-finite values. No bound on the sum of `occ_mask` or of `virt_mask` or of `chi_mask` on one device may be relied on, other than what follows from the above.
Results may differ from the reference program's by a relative error of at most 0.0029.
Values may be sent and summed in bfloat16 or wider, within the bound.
A program may use at most 64 MiB of HBM per device.

```python
import jax
import jax.numpy as jnp
from jax import lax

N = 8192
BLOCK = 128
ROWS = 1024
COLS = 2048
TAU = 8
FREQ = 8


def with_ends(values, rng, smallest, largest):
    longest = values.shape.index(max(values.shape))
    spots = []
    for shift in (0, 1):
        where = [jax.random.randint(jax.random.fold_in(rng, axis), (), 0, length) for axis, length in enumerate(values.shape)]
        where[longest] = (where[longest] + shift) % values.shape[longest]
        spots.append(tuple(where))
    return values.at[spots[0]].set(smallest).at[spots[1]].set(largest)


def shard_levels(stream_key, dims, split, low, high):
    factor_of = 1.0
    for dim, blocks in split:
        steps = jax.random.uniform(jax.random.fold_in(jax.random.fold_in(stream_key, 6), dim), (blocks,), jnp.float32, low / len(split), high / len(split))
        factor_of = factor_of * jnp.repeat(jnp.exp(steps), dims[dim] // blocks).reshape((-1,) + (1,) * (len(dims) - 1 - dim))
    return factor_of


def centred(rng, extent, deviation, most, split=(), kind=jnp.bfloat16):
    factor_of = shard_levels(rng, extent, split, -0.22, 0.18) if split else 1.0
    values = jax.random.normal(rng, extent, jnp.float32) * deviation * factor_of
    return jnp.minimum(jnp.maximum(values, -most), most).astype(kind)


def setup_inputs(seed: int = 0) -> dict:
    seeds = jax.random.split(jax.random.key(seed), 7)
    return {
        "occupied": centred(seeds[0], (TAU, ROWS, N), 1.0, 6.0, ((0, 8), (1, 8), (2, 8))),
        "virtual_green": centred(seeds[1], (TAU, N, COLS), N ** -0.5, 0.0625, ((0, 8), (1, 8), (2, 8))),
        "occ_mask": with_ends((jax.random.randint(seeds[2], (ROWS // BLOCK, N // BLOCK), 0, 4) < 3).astype(jnp.int32), jax.random.fold_in(seeds[2], 1), 0, 1),
        "virt_mask": with_ends((jax.random.randint(seeds[3], (N // BLOCK, COLS // BLOCK), 0, 4) < 3).astype(jnp.int32), jax.random.fold_in(seeds[3], 1), 0, 1),
        "chi_mask": with_ends((jax.random.randint(seeds[4], (ROWS // BLOCK, COLS // BLOCK), 0, 3) < 2).astype(jnp.int32), jax.random.fold_in(seeds[4], 1), 0, 1),
        "cosine_weights": centred(seeds[5], (FREQ, TAU), 0.5, 3.0, (), jnp.float32),
    }


def expand_mask(values, flags):
    block_rows = values.shape[0] // flags.shape[0]
    block_cols = values.shape[1] // flags.shape[1]
    shaped = values.reshape(flags.shape[0], block_rows, flags.shape[1], block_cols)
    masked = shaped * flags.astype(values.dtype)[:, None, :, None]
    return masked.reshape(values.shape)


def reference(occupied, virtual_green, occ_mask, virt_mask, chi_mask, cosine_weights):
    def one_time(pair):
        occ_slab, virt_slab = pair
        product = jnp.dot(expand_mask(occ_slab, occ_mask), expand_mask(virt_slab, virt_mask), preferred_element_type=jnp.float32)
        return expand_mask(product, chi_mask).astype(jnp.bfloat16)

    chi_tau = lax.map(one_time, (occupied, virtual_green))
    return jnp.einsum("kt,tij->kij", cosine_weights.astype(jnp.float32), chi_tau.astype(jnp.float32), precision=lax.Precision.HIGHEST)
```

```python
import functools

import jax
import jax.numpy as jnp
from jax import lax
from jax.experimental import pallas as pl
from jax.experimental.pallas import tpu as pltpu
from jax.sharding import PartitionSpec as P

MESH = pl.DeviceIdType.MESH
CH = 8
OFFS = (1, 3, 2)


def kernel(
    occ_hbm, virt_hbm, occ_mask, virt_mask, chi_mask, weights, out_ref,
    occ, virt, acc, chi, regroup,
    load_sem, z_sem, x_sem, xc_sem, y_sem, d_sem, t_sem, right_sem, left_sem,
):
    tau = lax.axis_index("tau")
    row = lax.axis_index("row")
    col = lax.axis_index("col")
    y, core = row // 2, lax.rem(row, 2)
    x, half = col // 2, lax.rem(col, 2)
    mine = col
    cross = x * 2 + 1 - half

    def x_peer(o):
        return (tau, row, lax.rem(x + o, 4) * 2 + half)

    def y_peer(o):
        return (tau, lax.rem(y + o, 4) * 2 + core, col)

    partner = (tau, y * 2 + 1 - core, col)
    across = (tau, row, cross)

    loads = [
        pltpu.make_async_copy(
            occ_hbm.at[0, :, pl.ds(c * 128, 128)], occ.at[mine, c], load_sem.at[c]
        )
        for c in range(CH)
    ]
    loads.append(pltpu.make_async_copy(virt_hbm.at[0], virt.at[row], load_sem.at[CH]))
    for load in loads:
        load.start()

    barrier = pltpu.get_barrier_semaphore()
    for peer in [x_peer(o) for o in OFFS] + [y_peer(o) for o in OFFS] + [partner, across]:
        pl.semaphore_signal(barrier, inc=1, device_id=peer, device_id_type=MESH)

    @pl.when(tau < 7)
    def _():
        pl.semaphore_signal(barrier, inc=1, device_id=(tau + 1, row, col), device_id_type=MESH)

    @pl.when(tau > 0)
    def _():
        pl.semaphore_signal(barrier, inc=1, device_id=(tau - 1, row, col), device_id_type=MESH)

    for c in range(CH):
        loads[c].wait()
        flag = occ_mask[0, c].astype(jnp.float32)
        occ[mine, c] = (occ[mine, c].astype(jnp.float32) * flag).astype(jnp.bfloat16)
    loads[CH].wait()
    for i in range(8):
        for j in range(2):
            flag = virt_mask[i, j].astype(jnp.float32)
            block = virt[row, pl.ds(i * 128, 128), pl.ds(j * 128, 128)]
            virt[row, pl.ds(i * 128, 128), pl.ds(j * 128, 128)] = (
                block.astype(jnp.float32) * flag
            ).astype(jnp.bfloat16)

    ends = jnp.where(tau == 0, 1, 0) + jnp.where(tau == 7, 1, 0)
    pl.semaphore_wait(barrier, 10 - ends)

    def remote(src, dst, sems, at, peer):
        return pltpu.make_async_remote_copy(
            src_ref=src, dst_ref=dst, send_sem=sems.at[(0, *at)], recv_sem=sems.at[(1, *at)],
            device_id=peer, device_id_type=MESH,
        )

    def z_copy(c):
        return remote(occ.at[mine, c], occ.at[mine, c], z_sem, (c,), across)

    def x_copy(i):
        return remote(occ.at[mine], occ.at[mine], x_sem, (i,), x_peer(OFFS[i]))

    def xc_copy(c, i):
        return remote(occ.at[cross, c], occ.at[cross, c], xc_sem, (c, i), x_peer(OFFS[i]))

    def y_copy(i):
        return remote(virt.at[row], virt.at[row], y_sem, (i,), y_peer(OFFS[i]))

    def d_copy(i):
        r = row if i == 0 else lax.rem(y + 4 - OFFS[i - 1], 4) * 2 + core
        return remote(virt.at[r], virt.at[r], d_sem, (i,), partner)

    def t_copy(o):
        to = lax.rem(tau + o, 8)
        return remote(chi.at[to], regroup.at[tau], t_sem, (o - 1,), (to, row, col))

    for c in range(CH):
        z_copy(c).start()
    for i in range(3):
        x_copy(i).start()
        y_copy(i).start()
        if i == 0:
            d_copy(0).start()

    @pl.when(tau > 0)
    def _():
        pl.semaphore_wait(right_sem, 1)

    @pl.when(tau < 7)
    def _():
        pl.semaphore_signal(right_sem, inc=1, device_id=(tau + 1, row, col), device_id_type=MESH)
        pl.semaphore_wait(left_sem, 1)

    @pl.when(tau > 0)
    def _():
        pl.semaphore_signal(left_sem, inc=1, device_id=(tau - 1, row, col), device_id_type=MESH)

    def dot_chunks(kb, first, count):
        total = None
        for c in range(first, first + count, 2):
            lhs = jnp.concatenate([occ[kb, c], occ[kb, c + 1]], axis=1)
            rhs = virt[kb, pl.ds(c * 128, 256), :]
            part = jnp.dot(lhs, rhs, preferred_element_type=jnp.float32)
            total = part if total is None else total + part
        return total

    def block_of(o, h):
        return lax.rem(y + 4 - o, 4) * 2 + h

    def own_half(o):
        acc[...] += dot_chunks(block_of(o, half), 0, CH)

    def cross_half(o, first, count):
        acc[...] += dot_chunks(block_of(o, 1 - half), first, count)

    def z_arrived(c):
        z_copy(c).wait_recv()
        for i in range(3):
            xc_copy(c, i).start()

    def y_arrived(i):
        y_copy(i).wait_recv()
        d_copy(i + 1).start()

    def xc_arrived(c):
        for i in range(3):
            xc_copy(c, i).wait_recv()

    acc[...] = jnp.zeros_like(acc)
    z_arrived(0)
    z_arrived(1)
    z_arrived(2)
    d_copy(0).wait_recv()
    for i in range(3):
        x_copy(i).wait_recv()
    own_half(0)
    y_arrived(0)
    y_arrived(1)
    z_arrived(3)
    d_copy(1).wait_recv()
    own_half(1)
    d_copy(2).wait_recv()
    own_half(3)
    z_arrived(4)
    for pair in (0, 2):
        xc_arrived(pair)
        xc_arrived(pair + 1)
        for o in (0, 1, 3):
            cross_half(o, pair, 2)
    z_arrived(5)
    z_arrived(6)
    z_arrived(7)
    y_arrived(2)
    xc_arrived(4)
    xc_arrived(5)
    for o in (0, 1, 3):
        cross_half(o, 4, 2)
    d_copy(3).wait_recv()
    own_half(2)
    cross_half(2, 0, 6)
    xc_arrived(6)
    xc_arrived(7)
    for o in (0, 1, 3, 2):
        cross_half(o, 6, 2)

    for j in range(2):
        flag = chi_mask[0, j].astype(jnp.float32)
        cols = pl.ds(j * 128, 128)
        chi[:, :, cols] = (acc[:, cols] * flag).astype(jnp.bfloat16).reshape(8, 16, 128)
    for o in (4, 5, 3, 6, 2, 7, 1):
        t_copy(o).start()
    regroup[tau] = chi[tau]
    for o in (1, 7, 2, 6, 3, 5, 4):
        t_copy(o).wait_recv()
    slices = [regroup[t].astype(jnp.float32) for t in range(8)]
    for k in range(8):
        total = slices[0] * weights[k, 0]
        for t in range(1, 8):
            total = total + slices[t] * weights[k, t]
        out_ref[k] = total

    for c in range(CH):
        z_copy(c).wait_send()
        for i in range(3):
            xc_copy(c, i).wait_send()
    for i in range(3):
        x_copy(i).wait_send()
        y_copy(i).wait_send()
    for i in range(4):
        d_copy(i).wait_send()
    for o in range(1, 8):
        t_copy(o).wait_send()


def shards(occupied, virtual_green, occ_mask, virt_mask, chi_mask, cosine_weights):
    smem = pl.BlockSpec(memory_space=pltpu.SMEM)
    hbm = pl.BlockSpec(memory_space=pl.ANY)
    dma = pltpu.SemaphoreType.DMA
    return pl.pallas_call(
        kernel,
        out_shape=jax.ShapeDtypeStruct((8, 16, 256), jnp.float32),
        in_specs=[hbm, hbm, smem, smem, smem, smem],
        out_specs=pl.BlockSpec(memory_space=pltpu.VMEM),
        scratch_shapes=[
            pltpu.VMEM((8, CH, 128, 128), jnp.bfloat16),
            pltpu.VMEM((8, 1024, 256), jnp.bfloat16),
            pltpu.VMEM((128, 256), jnp.float32),
            pltpu.VMEM((8, 16, 256), jnp.bfloat16),
            pltpu.VMEM((8, 16, 256), jnp.bfloat16),
            dma((CH + 1,)),
            dma((2, CH)),
            dma((2, 3)),
            dma((2, CH, 3)),
            dma((2, 3)),
            dma((2, 4)),
            dma((2, 7)),
            pltpu.SemaphoreType.REGULAR,
            pltpu.SemaphoreType.REGULAR,
        ],
        compiler_params=pltpu.CompilerParams(collective_id=0, has_side_effects=True),
        name="polarizability",
    )(occupied, virtual_green, occ_mask, virt_mask, chi_mask, cosine_weights)


def solution(mesh):
    placed = (
        P("tau", "row", "col"),
        P("tau", "row", "col"),
        P("row", "col"),
        P("row", "col"),
        P("row", "col"),
        P(),
    )
    return jax.shard_map(
        shards,
        mesh=mesh,
        in_specs=placed,
        out_specs=P(None, ("row", "tau"), "col"),
        check_vma=False,
    )
```

```python
import functools

import jax
import jax.numpy as jnp
from jax import lax
from jax.experimental import pallas as pl
from jax.experimental.pallas import tpu as pltpu
from jax.sharding import PartitionSpec as P

MESH = pl.DeviceIdType.MESH
CH = 8
OFFS = (2, 1, 3)


def kernel(
    occ_hbm, virt_hbm, occ_mask_hbm, virt_mask_hbm, chi_mask_hbm, weights_hbm, out_ref,
    occ, virt, acc, chi, regroup, occ_mask, virt_mask, chi_mask, weights,
    load_sem, z_sem, x_sem, xc_sem, y_sem, d_sem, own_sem, t_sem, reach_sem,
):
    tau = lax.axis_index("tau")
    row = lax.axis_index("row")
    col = lax.axis_index("col")
    y, core = row // 2, lax.rem(row, 2)
    x, half = col // 2, lax.rem(col, 2)
    mine = col
    cross = x * 2 + 1 - half

    def x_peer(o):
        return (tau, row, lax.rem(x + o, 4) * 2 + half)

    def y_peer(o):
        return (tau, lax.rem(y + o, 4) * 2 + core, col)

    partner = (tau, y * 2 + 1 - core, col)
    across = (tau, row, cross)

    barrier = pltpu.get_barrier_semaphore()
    for peer in [x_peer(o) for o in OFFS] + [y_peer(1), y_peer(3), partner, across]:
        pl.semaphore_signal(barrier, inc=1, device_id=peer, device_id_type=MESH)

    @pl.when(tau < 7)
    def _():
        pl.semaphore_signal(barrier, inc=1, device_id=(tau + 1, row, col), device_id_type=MESH)

    @pl.when(tau > 0)
    def _():
        pl.semaphore_signal(barrier, inc=1, device_id=(tau - 1, row, col), device_id_type=MESH)

    loads = [
        pltpu.make_async_copy(
            occ_hbm.at[0, :, pl.ds(c * 128, 128)], occ.at[mine, c], load_sem.at[c]
        )
        for c in range(CH)
    ]
    loads.append(pltpu.make_async_copy(virt_hbm.at[0], virt.at[row], load_sem.at[CH]))
    small = [
        pltpu.make_async_copy(src, dst, load_sem.at[CH + 1 + i])
        for i, (src, dst) in enumerate(
            [
                (occ_mask_hbm, occ_mask),
                (virt_mask_hbm, virt_mask),
                (chi_mask_hbm, chi_mask),
                (weights_hbm, weights),
            ]
        )
    ]
    small[0].start()
    for load in loads:
        load.start()
    for load in small[1:]:
        load.start()

    small[0].wait()
    for c in range(CH):
        loads[c].wait()
        flag = occ_mask[0, c].astype(jnp.float32)
        occ[mine, c] = (occ[mine, c].astype(jnp.float32) * flag).astype(jnp.bfloat16)
    ends = jnp.where(tau == 0, 1, 0) + jnp.where(tau == 7, 1, 0)
    pl.semaphore_wait(barrier, 9 - ends)

    def remote(src, dst, sems, at, peer):
        return pltpu.make_async_remote_copy(
            src_ref=src, dst_ref=dst, send_sem=sems.at[(0, *at)], recv_sem=sems.at[(1, *at)],
            device_id=peer, device_id_type=MESH,
        )

    def z_copy(c):
        return remote(occ.at[mine, c], occ.at[mine, c], z_sem, (c,), across)

    def x_copy(i):
        return remote(occ.at[mine], occ.at[mine], x_sem, (i,), x_peer(OFFS[i]))

    def xc_copy(c, i):
        return remote(occ.at[cross, c], occ.at[cross, c], xc_sem, (c, i), x_peer(OFFS[i]))

    def quarter(r, way, k):
        return virt.at[r, pl.ds(512 * ((way + k // 2) % 2) + 256 * (k % 2), 256)]

    def y_copy(way, k):
        r = row if k < 4 else lax.rem(y + 3 - 2 * way, 4) * 2 + core
        part = quarter(r, way, k)
        return remote(part, part, y_sem, (way, k), y_peer(1 + 2 * way))

    def d_copy(way, k):
        r = lax.rem(y + (3 - 2 * way if k < 4 else 2), 4) * 2 + core
        part = quarter(r, way, k)
        return remote(part, part, d_sem, (way, k), partner)

    def own_copy():
        return remote(virt.at[row], virt.at[row], own_sem, (), partner)

    def t_copy(o):
        to = lax.rem(tau + o, 8)
        return remote(chi.at[to], regroup.at[tau], t_sem, (o - 1,), (to, row, col))

    for c in range(2):
        z_copy(c).start()
    for i in range(3):
        x_copy(i).start()
    loads[CH].wait()
    small[1].wait()
    for i in range(8):
        for j in range(2):
            flag = virt_mask[j, i].astype(jnp.float32)
            block = virt[row, pl.ds(i * 128, 128), pl.ds(j * 128, 128)]
            virt[row, pl.ds(i * 128, 128), pl.ds(j * 128, 128)] = (
                block.astype(jnp.float32) * flag
            ).astype(jnp.bfloat16)

    for k in range(4):
        for way in range(2):
            y_copy(way, k).start()
    own_copy().start()
    small[2].wait()
    small[3].wait()

    def tell(k):
        for step in (-(2**k), 2**k):
            @pl.when(jnp.logical_and(tau + step >= 0, tau + step < 8))
            def _():
                pl.semaphore_signal(
                    reach_sem.at[k], inc=1, device_id=(tau + step, row, col), device_id_type=MESH
                )

    def hear(k):
        below, above = jnp.where(tau >= 2**k, 1, 0), jnp.where(tau < 8 - 2**k, 1, 0)
        pl.semaphore_wait(reach_sem.at[k], below + above)

    tell(0)

    def dot_chunks(kb, first, count):
        total = None
        for c in range(first, first + count, 2):
            lhs = jnp.concatenate([occ[kb, c], occ[kb, c + 1]], axis=1)
            rhs = virt[kb, pl.ds(c * 128, 256), :]
            part = jnp.dot(lhs, rhs, preferred_element_type=jnp.float32)
            total = part if total is None else total + part
        return total

    def block_of(o, h):
        return lax.rem(y + 4 - o, 4) * 2 + h

    def own_half(o):
        acc[...] += dot_chunks(block_of(o, half), 0, CH)

    def cross_half(o, first, count):
        acc[...] += dot_chunks(block_of(o, 1 - half), first, count)

    def z_arrived(c):
        z_copy(c).wait_recv()
        for i in range(3):
            xc_copy(c, i).start()

    def y_arrived(k):
        for way in range(2):
            y_copy(way, k).wait_recv()
            if k < 2:
                y_copy(way, k + 4).start()
            d_copy(way, k).start()
        z_copy(k + 2).start()

    def d_arrived(k):
        for way in range(2):
            d_copy(way, k).wait_recv()

    def xc_arrived(c):
        for i in range(3):
            xc_copy(c, i).wait_recv()

    acc[...] = jnp.zeros_like(acc)
    y_arrived(0)
    y_arrived(1)
    hear(0)
    tell(1)
    y_arrived(2)
    z_arrived(0)
    y_arrived(3)
    z_arrived(1)
    y_arrived(4)
    z_arrived(2)
    y_arrived(5)
    hear(1)
    tell(2)
    z_arrived(3)
    own_copy().wait_recv()
    for i in range(3):
        x_copy(i).wait_recv()
    own_half(0)
    z_arrived(4)
    for k in range(4):
        d_arrived(k)
    own_half(1)
    own_half(3)
    z_arrived(5)
    d_arrived(4)
    d_arrived(5)
    own_half(2)
    hear(2)
    z_arrived(6)
    for pair in (0, 2):
        xc_arrived(pair)
        xc_arrived(pair + 1)
        for o in range(4):
            cross_half(o, pair, 2)
    z_arrived(7)
    for pair in (4, 6):
        xc_arrived(pair)
        xc_arrived(pair + 1)
        for o in range(4):
            cross_half(o, pair, 2)

    for j in range(2):
        flag = chi_mask[0, j].astype(jnp.float32)
        cols = pl.ds(j * 128, 128)
        chi[:, :, cols] = (acc[:, cols] * flag).astype(jnp.bfloat16).reshape(8, 16, 128)
    for o in (4, 5, 3, 6, 2, 7, 1):
        t_copy(o).start()
    regroup[tau] = chi[tau]
    for o in (1, 7, 2, 6, 3, 5, 4):
        t_copy(o).wait_recv()
    slices = [regroup[t].astype(jnp.float32) for t in range(8)]
    for k in range(8):
        total = slices[0] * weights[k, 0]
        for t in range(1, 8):
            total = total + slices[t] * weights[k, t]
        out_ref[k] = total

    for c in range(CH):
        z_copy(c).wait_send()
        for i in range(3):
            xc_copy(c, i).wait_send()
    for i in range(3):
        x_copy(i).wait_send()
    for k in range(6):
        for way in range(2):
            y_copy(way, k).wait_send()
            d_copy(way, k).wait_send()
    own_copy().wait_send()
    for o in range(1, 8):
        t_copy(o).wait_send()


def shards(occupied, virtual_green, occ_mask, virt_mask, chi_mask, cosine_weights):
    dma = pltpu.SemaphoreType.DMA
    return pl.pallas_call(
        kernel,
        out_shape=jax.ShapeDtypeStruct((8, 16, 256), jnp.float32),
        in_specs=[pl.BlockSpec(memory_space=pl.ANY)] * 6,
        out_specs=pl.BlockSpec(memory_space=pltpu.VMEM),
        scratch_shapes=[
            pltpu.VMEM((8, CH, 128, 128), jnp.bfloat16),
            pltpu.VMEM((8, 1024, 256), jnp.bfloat16),
            pltpu.VMEM((128, 256), jnp.float32),
            pltpu.VMEM((8, 16, 256), jnp.bfloat16),
            pltpu.VMEM((8, 16, 256), jnp.bfloat16),
            pltpu.SMEM((1, 8), jnp.int32),
            pltpu.SMEM((2, 8), jnp.int32),
            pltpu.SMEM((1, 2), jnp.int32),
            pltpu.SMEM((8, 8), jnp.float32),
            dma((CH + 5,)),
            dma((2, CH)),
            dma((2, 3)),
            dma((2, CH, 3)),
            dma((2, 2, 6)),
            dma((2, 2, 6)),
            dma((2,)),
            dma((2, 7)),
            pltpu.SemaphoreType.REGULAR((3,)),
        ],
        compiler_params=pltpu.CompilerParams(collective_id=0, has_side_effects=True),
        name="polarizability",
    )(occupied, virtual_green, occ_mask, virt_mask.T, chi_mask, cosine_weights)


def solution(mesh):
    placed = (
        P("tau", "row", "col"),
        P("tau", "row", "col"),
        P("row", "col"),
        P("row", "col"),
        P("row", "col"),
        P(),
    )
    return jax.shard_map(
        shards,
        mesh=mesh,
        in_specs=placed,
        out_specs=P(None, ("row", "tau"), "col"),
        check_vma=False,
    )
```

```python
import functools

import jax
import jax.numpy as jnp
from jax import lax
from jax.experimental import pallas as pl
from jax.experimental.pallas import tpu as pltpu
from jax.sharding import PartitionSpec as P

MESH = pl.DeviceIdType.MESH
CH = 8
PIECES = [(c, 0, 128) for c in range(7)] + [(7, 0, 64), (7, 64, 64)]
AHEAD = (3, 3)
OFFS = (2, 1, 3)


def kernel(
    occ_hbm, virt_hbm, occ_mask_hbm, virt_mask_hbm, chi_mask_hbm, weights_hbm, out_ref,
    occ, virt, acc, chi, regroup, occ_mask, virt_mask, chi_mask, weights,
    load_sem, z_sem, x_sem, xc_sem, y_sem, d_sem, own_sem, t_sem, reach_sem,
):
    tau = lax.axis_index("tau")
    row = lax.axis_index("row")
    col = lax.axis_index("col")
    y, core = row // 2, lax.rem(row, 2)
    x, half = col // 2, lax.rem(col, 2)
    mine = col
    cross = x * 2 + 1 - half

    def x_peer(o):
        return (tau, row, lax.rem(x + o, 4) * 2 + half)

    def y_peer(o):
        return (tau, lax.rem(y + o, 4) * 2 + core, col)

    partner = (tau, y * 2 + 1 - core, col)
    across = (tau, row, cross)

    barrier = pltpu.get_barrier_semaphore()
    for peer in [x_peer(o) for o in OFFS] + [y_peer(1), y_peer(3), partner, across]:
        pl.semaphore_signal(barrier, inc=1, device_id=peer, device_id_type=MESH)

    @pl.when(tau < 7)
    def _():
        pl.semaphore_signal(barrier, inc=1, device_id=(tau + 1, row, col), device_id_type=MESH)

    @pl.when(tau > 0)
    def _():
        pl.semaphore_signal(barrier, inc=1, device_id=(tau - 1, row, col), device_id_type=MESH)

    loads = [
        pltpu.make_async_copy(
            occ_hbm.at[0, :, pl.ds(c * 128, 128)], occ.at[mine, c], load_sem.at[c]
        )
        for c in range(CH)
    ]
    loads.append(pltpu.make_async_copy(virt_hbm.at[0], virt.at[row], load_sem.at[CH]))
    small = [
        pltpu.make_async_copy(src, dst, load_sem.at[CH + 1 + i])
        for i, (src, dst) in enumerate(
            [
                (occ_mask_hbm, occ_mask),
                (virt_mask_hbm, virt_mask),
                (chi_mask_hbm, chi_mask),
                (weights_hbm, weights),
            ]
        )
    ]
    small[0].start()
    for load in loads:
        load.start()
    for load in small[1:]:
        load.start()

    small[0].wait()
    for c in range(CH):
        loads[c].wait()
        flag = occ_mask[0, c].astype(jnp.float32)
        occ[mine, c] = (occ[mine, c].astype(jnp.float32) * flag).astype(jnp.bfloat16)
    ends = jnp.where(tau == 0, 1, 0) + jnp.where(tau == 7, 1, 0)
    pl.semaphore_wait(barrier, 9 - ends)

    def remote(src, dst, sems, at, peer):
        return pltpu.make_async_remote_copy(
            src_ref=src, dst_ref=dst, send_sem=sems.at[(0, *at)], recv_sem=sems.at[(1, *at)],
            device_id=peer, device_id_type=MESH,
        )

    def piece(kb, p):
        c, first, count = PIECES[p]
        return occ.at[kb, c, pl.ds(first, count)]

    def z_copy(p):
        return remote(piece(mine, p), piece(mine, p), z_sem, (p,), across)

    def z_start(half_is, p):
        if p < len(PIECES):
            @pl.when(half == half_is)
            def _():
                z_copy(p).start()

    def x_copy(i):
        return remote(occ.at[mine], occ.at[mine], x_sem, (i,), x_peer(OFFS[i]))

    def xc_copy(p, i):
        return remote(piece(cross, p), piece(cross, p), xc_sem, (p, i), x_peer(OFFS[i]))

    def quarter(r, way, k):
        return virt.at[r, pl.ds(512 * ((way + k // 2) % 2) + 256 * (k % 2), 256)]

    def y_copy(way, k):
        r = row if k < 4 else lax.rem(y + 3 - 2 * way, 4) * 2 + core
        part = quarter(r, way, k)
        return remote(part, part, y_sem, (way, k), y_peer(1 + 2 * way))

    def d_copy(way, k):
        r = lax.rem(y + (3 - 2 * way if k < 4 else 2), 4) * 2 + core
        part = quarter(r, way, k)
        return remote(part, part, d_sem, (way, k), partner)

    def own_copy():
        return remote(virt.at[row], virt.at[row], own_sem, (), partner)

    def t_copy(to, sender):
        return pltpu.make_async_remote_copy(
            src_ref=chi.at[to], dst_ref=regroup.at[tau],
            send_sem=t_sem.at[0, to], recv_sem=t_sem.at[1, sender],
            device_id=(to, row, col), device_id_type=MESH,
        )

    for h in range(2):
        for p in range(AHEAD[h]):
            z_start(h, p)
    for i in range(3):
        x_copy(i).start()
    loads[CH].wait()
    small[1].wait()
    for i in range(8):
        for j in range(2):
            flag = virt_mask[j, i].astype(jnp.float32)
            block = virt[row, pl.ds(i * 128, 128), pl.ds(j * 128, 128)]
            virt[row, pl.ds(i * 128, 128), pl.ds(j * 128, 128)] = (
                block.astype(jnp.float32) * flag
            ).astype(jnp.bfloat16)

    for k in range(4):
        for way in range(2):
            y_copy(way, k).start()
    own_copy().start()
    small[2].wait()
    small[3].wait()

    def tell(k):
        for step in (-(2**k), 2**k):
            @pl.when(jnp.logical_and(tau + step >= 0, tau + step < 8))
            def _():
                pl.semaphore_signal(
                    reach_sem.at[k], inc=1, device_id=(tau + step, row, col), device_id_type=MESH
                )

    def hear(k):
        below, above = jnp.where(tau >= 2**k, 1, 0), jnp.where(tau < 8 - 2**k, 1, 0)
        pl.semaphore_wait(reach_sem.at[k], below + above)

    tell(0)

    def dot_chunks(kb, first, count):
        total = None
        for c in range(first, first + count, 2):
            lhs = jnp.concatenate([occ[kb, c], occ[kb, c + 1]], axis=1)
            rhs = virt[kb, pl.ds(c * 128, 256), :]
            part = jnp.dot(lhs, rhs, preferred_element_type=jnp.float32)
            total = part if total is None else total + part
        return total

    def block_of(o, h):
        return lax.rem(y + 4 - o, 4) * 2 + h

    def own_half(o):
        acc[...] += dot_chunks(block_of(o, half), 0, CH)

    def cross_half(o, first, count):
        acc[...] += dot_chunks(block_of(o, 1 - half), first, count)

    def z_arrived(c):
        z_copy(c).wait_recv()
        for i in range(3):
            xc_copy(c, i).start()

    def y_arrived(k):
        for way in range(2):
            y_copy(way, k).wait_recv()
            if k < 2:
                y_copy(way, k + 4).start()
            d_copy(way, k).start()
        for h in range(2):
            z_start(h, AHEAD[h] + k)
            if k == 5:
                for p in range(AHEAD[h] + 6, len(PIECES)):
                    z_start(h, p)

    def d_arrived(k):
        for way in range(2):
            d_copy(way, k).wait_recv()

    def xc_arrived(c):
        for i in range(3):
            xc_copy(c, i).wait_recv()

    acc[...] = jnp.zeros_like(acc)
    y_arrived(0)
    y_arrived(1)
    hear(0)
    tell(1)
    y_arrived(2)
    z_arrived(0)
    y_arrived(3)
    z_arrived(1)
    y_arrived(4)
    z_arrived(2)
    y_arrived(5)
    hear(1)
    tell(2)
    z_arrived(3)
    own_copy().wait_recv()
    for i in range(3):
        x_copy(i).wait_recv()
    own_half(0)
    z_arrived(4)
    for k in range(4):
        d_arrived(k)
    own_half(1)
    own_half(3)
    z_arrived(5)
    d_arrived(4)
    d_arrived(5)
    own_half(2)
    hear(2)
    z_arrived(6)
    for pair in (0, 2):
        xc_arrived(pair)
        xc_arrived(pair + 1)
        for o in range(4):
            cross_half(o, pair, 2)
    z_arrived(7)
    z_arrived(8)
    for pair in (4, 6):
        xc_arrived(pair)
        xc_arrived(pair + 1)
        if pair == 6:
            xc_arrived(8)
        for o in range(4):
            cross_half(o, pair, 2)

    for j in range(2):
        flag = chi_mask[0, j].astype(jnp.float32)
        cols = pl.ds(j * 128, 128)
        chi[:, :, cols] = (acc[:, cols] * flag).astype(jnp.bfloat16).reshape(8, 16, 128)
    for distance in range(7, 0, -1):
        for to in (tau + distance, tau - distance):
            @pl.when(jnp.logical_and(to >= 0, to < 8))
            def _():
                t_copy(to, tau).start()

    regroup[tau] = chi[tau]
    for o in range(1, 8):
        peer = lax.rem(tau + o, 8)
        t_copy(peer, peer).wait_recv()
    slices = [regroup[t].astype(jnp.float32) for t in range(8)]
    for k in range(8):
        total = slices[0] * weights[k, 0]
        for t in range(1, 8):
            total = total + slices[t] * weights[k, t]
        out_ref[k] = total

    for p in range(len(PIECES)):
        z_copy(p).wait_send()
        for i in range(3):
            xc_copy(p, i).wait_send()
    for i in range(3):
        x_copy(i).wait_send()
    for k in range(6):
        for way in range(2):
            y_copy(way, k).wait_send()
            d_copy(way, k).wait_send()
    own_copy().wait_send()
    for o in range(1, 8):
        t_copy(lax.rem(tau + o, 8), tau).wait_send()


def shards(occupied, virtual_green, occ_mask, virt_mask, chi_mask, cosine_weights):
    dma = pltpu.SemaphoreType.DMA
    return pl.pallas_call(
        kernel,
        out_shape=jax.ShapeDtypeStruct((8, 16, 256), jnp.float32),
        in_specs=[pl.BlockSpec(memory_space=pl.ANY)] * 6,
        out_specs=pl.BlockSpec(memory_space=pltpu.VMEM),
        scratch_shapes=[
            pltpu.VMEM((8, CH, 128, 128), jnp.bfloat16),
            pltpu.VMEM((8, 1024, 256), jnp.bfloat16),
            pltpu.VMEM((128, 256), jnp.float32),
            pltpu.VMEM((8, 16, 256), jnp.bfloat16),
            pltpu.VMEM((8, 16, 256), jnp.bfloat16),
            pltpu.SMEM((1, 8), jnp.int32),
            pltpu.SMEM((2, 8), jnp.int32),
            pltpu.SMEM((1, 2), jnp.int32),
            pltpu.SMEM((8, 8), jnp.float32),
            dma((CH + 5,)),
            dma((2, len(PIECES))),
            dma((2, 3)),
            dma((2, len(PIECES), 3)),
            dma((2, 2, 6)),
            dma((2, 2, 6)),
            dma((2,)),
            dma((2, 8)),
            pltpu.SemaphoreType.REGULAR((3,)),
        ],
        compiler_params=pltpu.CompilerParams(collective_id=0, has_side_effects=True),
        name="polarizability",
    )(occupied, virtual_green, occ_mask, virt_mask.T, chi_mask, cosine_weights)


def solution(mesh):
    placed = (
        P("tau", "row", "col"),
        P("tau", "row", "col"),
        P("row", "col"),
        P("row", "col"),
        P("row", "col"),
        P(),
    )
    return jax.shard_map(
        shards,
        mesh=mesh,
        in_specs=placed,
        out_specs=P(None, ("row", "tau"), "col"),
        check_vma=False,
    )
```

```python
import functools

import jax
import jax.numpy as jnp
from jax import lax
from jax.experimental import pallas as pl
from jax.experimental.pallas import tpu as pltpu
from jax.sharding import PartitionSpec as P

MESH = pl.DeviceIdType.MESH
CH = 8
AHEAD = 3
OFFS = (2, 1, 3)


def kernel(
    occ_hbm, virt_hbm, occ_mask_hbm, virt_mask_hbm, chi_mask_hbm, weights_hbm, out_ref,
    occ, virt, acc, chi, regroup, occ_mask, virt_mask, chi_mask, weights,
    load_sem, z_sem, x_sem, xc_sem, y_sem, d_sem, own_sem, t_sem, reach_sem,
):
    tau = lax.axis_index("tau")
    row = lax.axis_index("row")
    col = lax.axis_index("col")
    y, core = row // 2, lax.rem(row, 2)
    x, half = col // 2, lax.rem(col, 2)
    mine = col
    cross = x * 2 + 1 - half

    def x_peer(o):
        return (tau, row, lax.rem(x + o, 4) * 2 + half)

    def y_peer(o):
        return (tau, lax.rem(y + o, 4) * 2 + core, col)

    partner = (tau, y * 2 + 1 - core, col)
    across = (tau, row, cross)

    barrier = pltpu.get_barrier_semaphore()
    for peer in [x_peer(o) for o in OFFS] + [y_peer(1), y_peer(3), partner, across]:
        pl.semaphore_signal(barrier, inc=1, device_id=peer, device_id_type=MESH)

    @pl.when(tau < 7)
    def _():
        pl.semaphore_signal(barrier, inc=1, device_id=(tau + 1, row, col), device_id_type=MESH)

    @pl.when(tau > 0)
    def _():
        pl.semaphore_signal(barrier, inc=1, device_id=(tau - 1, row, col), device_id_type=MESH)

    loads = [
        pltpu.make_async_copy(
            occ_hbm.at[0, :, pl.ds(c * 128, 128)], occ.at[mine, c], load_sem.at[c]
        )
        for c in range(CH)
    ]
    loads.append(pltpu.make_async_copy(virt_hbm.at[0], virt.at[row], load_sem.at[CH]))
    small = [
        pltpu.make_async_copy(src, dst, load_sem.at[CH + 1 + i])
        for i, (src, dst) in enumerate(
            [
                (occ_mask_hbm, occ_mask),
                (virt_mask_hbm, virt_mask),
                (chi_mask_hbm, chi_mask),
                (weights_hbm, weights),
            ]
        )
    ]
    small[0].start()
    for load in loads:
        load.start()
    for load in small[1:]:
        load.start()

    small[0].wait()
    for c in range(CH):
        loads[c].wait()
        flag = occ_mask[0, c].astype(jnp.float32)
        occ[mine, c] = (occ[mine, c].astype(jnp.float32) * flag).astype(jnp.bfloat16)
    ends = jnp.where(tau == 0, 1, 0) + jnp.where(tau == 7, 1, 0)
    pl.semaphore_wait(barrier, 9 - ends)

    def remote(src, dst, sems, at, peer):
        return pltpu.make_async_remote_copy(
            src_ref=src, dst_ref=dst, send_sem=sems.at[(0, *at)], recv_sem=sems.at[(1, *at)],
            device_id=peer, device_id_type=MESH,
        )

    def z_copy(c):
        return remote(occ.at[mine, c], occ.at[mine, c], z_sem, (c,), across)

    def x_copy(i):
        return remote(occ.at[mine], occ.at[mine], x_sem, (i,), x_peer(OFFS[i]))

    def xc_copy(c, i):
        return remote(occ.at[cross, c], occ.at[cross, c], xc_sem, (c, i), x_peer(OFFS[i]))

    def quarter(r, way, k):
        return virt.at[r, pl.ds(512 * ((way + k // 2) % 2) + 256 * (k % 2), 256)]

    def y_copy(way, k):
        r = row if k < 4 else lax.rem(y + 3 - 2 * way, 4) * 2 + core
        part = quarter(r, way, k)
        return remote(part, part, y_sem, (way, k), y_peer(1 + 2 * way))

    def d_copy(way, k):
        r = lax.rem(y + (3 - 2 * way if k < 4 else 2), 4) * 2 + core
        part = quarter(r, way, k)
        return remote(part, part, d_sem, (way, k), partner)

    def own_copy():
        return remote(virt.at[row], virt.at[row], own_sem, (), partner)

    def t_copy(to, sender):
        return pltpu.make_async_remote_copy(
            src_ref=chi.at[to], dst_ref=regroup.at[tau],
            send_sem=t_sem.at[0, to], recv_sem=t_sem.at[1, sender],
            device_id=(to, row, col), device_id_type=MESH,
        )

    for c in range(AHEAD):
        z_copy(c).start()
    for i in range(3):
        x_copy(i).start()
    loads[CH].wait()
    small[1].wait()
    for i in range(8):
        for j in range(2):
            flag = virt_mask[j, i].astype(jnp.float32)
            block = virt[row, pl.ds(i * 128, 128), pl.ds(j * 128, 128)]
            virt[row, pl.ds(i * 128, 128), pl.ds(j * 128, 128)] = (
                block.astype(jnp.float32) * flag
            ).astype(jnp.bfloat16)

    for k in range(4):
        for way in range(2):
            y_copy(way, k).start()
    own_copy().start()
    small[2].wait()
    small[3].wait()

    def tell(k):
        for step in (-(2**k), 2**k):
            @pl.when(jnp.logical_and(tau + step >= 0, tau + step < 8))
            def _():
                pl.semaphore_signal(
                    reach_sem.at[k], inc=1, device_id=(tau + step, row, col), device_id_type=MESH
                )

    def hear(k):
        below, above = jnp.where(tau >= 2**k, 1, 0), jnp.where(tau < 8 - 2**k, 1, 0)
        pl.semaphore_wait(reach_sem.at[k], below + above)

    tell(0)

    def dot_chunks(kb, first, count):
        total = None
        for c in range(first, first + count, 2):
            lhs = jnp.concatenate([occ[kb, c], occ[kb, c + 1]], axis=1)
            rhs = virt[kb, pl.ds(c * 128, 256), :]
            part = jnp.dot(lhs, rhs, preferred_element_type=jnp.float32)
            total = part if total is None else total + part
        return total

    def block_of(o, h):
        return lax.rem(y + 4 - o, 4) * 2 + h

    def own_half(o):
        acc[...] += dot_chunks(block_of(o, half), 0, CH)

    def cross_half(o, first, count):
        acc[...] += dot_chunks(block_of(o, 1 - half), first, count)

    def z_arrived(c):
        z_copy(c).wait_recv()
        for i in range(3):
            xc_copy(c, i).start()

    def y_arrived(k):
        for way in range(2):
            y_copy(way, k).wait_recv()
            if k < 2:
                y_copy(way, k + 4).start()
            d_copy(way, k).start()
        if k + AHEAD < CH:
            z_copy(k + AHEAD).start()

    def d_arrived(k):
        for way in range(2):
            d_copy(way, k).wait_recv()

    def xc_arrived(c):
        for i in range(3):
            xc_copy(c, i).wait_recv()

    acc[...] = jnp.zeros_like(acc)
    y_arrived(0)
    y_arrived(1)
    hear(0)
    tell(1)
    y_arrived(2)
    z_arrived(0)
    y_arrived(3)
    z_arrived(1)
    y_arrived(4)
    z_arrived(2)
    y_arrived(5)
    hear(1)
    tell(2)
    z_arrived(3)
    own_copy().wait_recv()
    for i in range(3):
        x_copy(i).wait_recv()
    own_half(0)
    z_arrived(4)
    for k in range(4):
        d_arrived(k)
    own_half(1)
    own_half(3)
    z_arrived(5)
    d_arrived(4)
    d_arrived(5)
    own_half(2)
    hear(2)
    z_arrived(6)
    for pair in (0, 2):
        xc_arrived(pair)
        xc_arrived(pair + 1)
        for o in range(4):
            cross_half(o, pair, 2)
    z_arrived(7)
    for pair in (4, 6):
        xc_arrived(pair)
        xc_arrived(pair + 1)
        for o in range(4):
            cross_half(o, pair, 2)

    for j in range(2):
        flag = chi_mask[0, j].astype(jnp.float32)
        cols = pl.ds(j * 128, 128)
        chi[:, :, cols] = (acc[:, cols] * flag).astype(jnp.bfloat16).reshape(8, 16, 128)
    for distance in range(7, 0, -1):
        for to in (tau + distance, tau - distance):
            @pl.when(jnp.logical_and(to >= 0, to < 8))
            def _():
                t_copy(to, tau).start()

    regroup[tau] = chi[tau]
    for c in range(CH):
        z_copy(c).wait_send()
        for i in range(3):
            xc_copy(c, i).wait_send()
    for i in range(3):
        x_copy(i).wait_send()
    for k in range(6):
        for way in range(2):
            y_copy(way, k).wait_send()
            d_copy(way, k).wait_send()
    own_copy().wait_send()
    for o in range(1, 8):
        t_copy(lax.rem(tau + o, 8), tau).wait_send()
    for o in range(1, 8):
        peer = lax.rem(tau + o, 8)
        t_copy(peer, peer).wait_recv()
    slices = [regroup[t].astype(jnp.float32) for t in range(8)]
    for k in range(8):
        total = slices[0] * weights[k, 0]
        for t in range(1, 8):
            total = total + slices[t] * weights[k, t]
        out_ref[k] = total


def shards(occupied, virtual_green, occ_mask, virt_mask, chi_mask, cosine_weights):
    dma = pltpu.SemaphoreType.DMA
    return pl.pallas_call(
        kernel,
        out_shape=pltpu.VMEM((8, 16, 256), jnp.float32),
        in_specs=[pl.BlockSpec(memory_space=pl.ANY)] * 6,
        out_specs=pl.BlockSpec(memory_space=pltpu.VMEM),
        scratch_shapes=[
            pltpu.VMEM((8, CH, 128, 128), jnp.bfloat16),
            pltpu.VMEM((8, 1024, 256), jnp.bfloat16),
            pltpu.VMEM((128, 256), jnp.float32),
            pltpu.VMEM((8, 16, 256), jnp.bfloat16),
            pltpu.VMEM((8, 16, 256), jnp.bfloat16),
            pltpu.SMEM((1, 8), jnp.int32),
            pltpu.SMEM((2, 8), jnp.int32),
            pltpu.SMEM((1, 2), jnp.int32),
            pltpu.SMEM((8, 8), jnp.float32),
            dma((CH + 5,)),
            dma((2, CH)),
            dma((2, 3)),
            dma((2, CH, 3)),
            dma((2, 2, 6)),
            dma((2, 2, 6)),
            dma((2,)),
            dma((2, 8)),
            pltpu.SemaphoreType.REGULAR((3,)),
        ],
        compiler_params=pltpu.CompilerParams(collective_id=0, has_side_effects=True),
        name="polarizability",
    )(occupied, virtual_green, occ_mask, virt_mask.T, chi_mask, cosine_weights)


def solution(mesh):
    placed = (
        P("tau", "row", "col"),
        P("tau", "row", "col"),
        P("row", "col"),
        P("row", "col"),
        P("row", "col"),
        P(),
    )
    return jax.shard_map(
        shards,
        mesh=mesh,
        in_specs=placed,
        out_specs=P(None, ("row", "tau"), "col"),
        check_vma=False,
    )
```

```python
import functools

import jax
import jax.numpy as jnp
from jax import lax
from jax.experimental import pallas as pl
from jax.experimental.pallas import tpu as pltpu
from jax.sharding import PartitionSpec as P

MESH = pl.DeviceIdType.MESH
CH = 8
AHEAD = 3
OFFS = (2, 1, 3)


def kernel(
    occ_hbm, virt_hbm, occ_mask_hbm, virt_mask_hbm, chi_mask_hbm, weights_hbm, out_ref,
    occ, virt, acc, chi, regroup, occ_mask, virt_mask, chi_mask, weights,
    load_sem, z_sem, x_sem, xc_sem, y_sem, d_sem, own_sem, t_sem, reach_sem,
):
    tau = lax.axis_index("tau")
    row = lax.axis_index("row")
    col = lax.axis_index("col")
    y, core = row // 2, lax.rem(row, 2)
    x, half = col // 2, lax.rem(col, 2)
    mine = col
    cross = x * 2 + 1 - half

    def x_peer(o):
        return (tau, row, lax.rem(x + o, 4) * 2 + half)

    def y_peer(o):
        return (tau, lax.rem(y + o, 4) * 2 + core, col)

    partner = (tau, y * 2 + 1 - core, col)
    across = (tau, row, cross)

    barrier = pltpu.get_barrier_semaphore()
    for peer in [x_peer(o) for o in OFFS] + [y_peer(1), y_peer(3), partner, across]:
        pl.semaphore_signal(barrier, inc=1, device_id=peer, device_id_type=MESH)

    @pl.when(tau < 7)
    def _():
        pl.semaphore_signal(barrier, inc=1, device_id=(tau + 1, row, col), device_id_type=MESH)

    @pl.when(tau > 0)
    def _():
        pl.semaphore_signal(barrier, inc=1, device_id=(tau - 1, row, col), device_id_type=MESH)

    loads = [
        pltpu.make_async_copy(
            occ_hbm.at[0, :, pl.ds(c * 128, 128)], occ.at[mine, c], load_sem.at[c]
        )
        for c in range(CH)
    ]
    loads.append(pltpu.make_async_copy(virt_hbm.at[0], virt.at[row], load_sem.at[CH]))
    small = [
        pltpu.make_async_copy(src, dst, load_sem.at[CH + 1 + i])
        for i, (src, dst) in enumerate(
            [
                (occ_mask_hbm, occ_mask),
                (virt_mask_hbm, virt_mask),
                (chi_mask_hbm, chi_mask),
                (weights_hbm, weights),
            ]
        )
    ]
    small[0].start()
    for load in loads:
        load.start()
    for load in small[1:]:
        load.start()

    def masked(c):
        loads[c].wait()
        flag = occ_mask[0, c].astype(jnp.float32)
        occ[mine, c] = (occ[mine, c].astype(jnp.float32) * flag).astype(jnp.bfloat16)

    small[0].wait()
    for c in range(AHEAD):
        masked(c)
    ends = jnp.where(tau == 0, 1, 0) + jnp.where(tau == 7, 1, 0)
    pl.semaphore_wait(barrier, 9 - ends)

    def remote(src, dst, sems, at, peer):
        return pltpu.make_async_remote_copy(
            src_ref=src, dst_ref=dst, send_sem=sems.at[(0, *at)], recv_sem=sems.at[(1, *at)],
            device_id=peer, device_id_type=MESH,
        )

    def z_copy(c):
        return remote(occ.at[mine, c], occ.at[mine, c], z_sem, (c,), across)

    def x_copy(i):
        return remote(occ.at[mine], occ.at[mine], x_sem, (i,), x_peer(OFFS[i]))

    def xc_copy(c, i):
        return remote(occ.at[cross, c], occ.at[cross, c], xc_sem, (c, i), x_peer(OFFS[i]))

    def quarter(r, way, k):
        return virt.at[r, pl.ds(512 * ((way + k // 2) % 2) + 256 * (k % 2), 256)]

    def y_copy(way, k):
        r = row if k < 4 else lax.rem(y + 3 - 2 * way, 4) * 2 + core
        part = quarter(r, way, k)
        return remote(part, part, y_sem, (way, k), y_peer(1 + 2 * way))

    def d_copy(way, k):
        r = lax.rem(y + (3 - 2 * way if k < 4 else 2), 4) * 2 + core
        part = quarter(r, way, k)
        return remote(part, part, d_sem, (way, k), partner)

    def own_copy():
        return remote(virt.at[row], virt.at[row], own_sem, (), partner)

    def t_copy(to, sender):
        return pltpu.make_async_remote_copy(
            src_ref=chi.at[to], dst_ref=regroup.at[tau],
            send_sem=t_sem.at[0, to], recv_sem=t_sem.at[1, sender],
            device_id=(to, row, col), device_id_type=MESH,
        )

    for c in range(AHEAD):
        z_copy(c).start()
    for c in range(AHEAD, CH):
        masked(c)
    for i in range(3):
        x_copy(i).start()
    loads[CH].wait()
    small[1].wait()
    for i in range(8):
        for j in range(2):
            flag = virt_mask[j, i].astype(jnp.float32)
            block = virt[row, pl.ds(i * 128, 128), pl.ds(j * 128, 128)]
            virt[row, pl.ds(i * 128, 128), pl.ds(j * 128, 128)] = (
                block.astype(jnp.float32) * flag
            ).astype(jnp.bfloat16)

    for k in range(4):
        for way in range(2):
            y_copy(way, k).start()
    own_copy().start()
    small[2].wait()
    small[3].wait()

    def tell(k):
        for step in (-(2**k), 2**k):
            @pl.when(jnp.logical_and(tau + step >= 0, tau + step < 8))
            def _():
                pl.semaphore_signal(
                    reach_sem.at[k], inc=1, device_id=(tau + step, row, col), device_id_type=MESH
                )

    def hear(k):
        below, above = jnp.where(tau >= 2**k, 1, 0), jnp.where(tau < 8 - 2**k, 1, 0)
        pl.semaphore_wait(reach_sem.at[k], below + above)

    tell(0)

    def dot_chunks(kb, first, count):
        total = None
        for c in range(first, first + count, 2):
            lhs = jnp.concatenate([occ[kb, c], occ[kb, c + 1]], axis=1)
            rhs = virt[kb, pl.ds(c * 128, 256), :]
            part = jnp.dot(lhs, rhs, preferred_element_type=jnp.float32)
            total = part if total is None else total + part
        return total

    def block_of(o, h):
        return lax.rem(y + 4 - o, 4) * 2 + h

    def own_half(o):
        acc[...] += dot_chunks(block_of(o, half), 0, CH)

    def cross_half(o, first, count):
        acc[...] += dot_chunks(block_of(o, 1 - half), first, count)

    def last_cross(c):
        total = acc[...]
        for o in (0, 2):
            a, b = block_of(o, 1 - half), block_of(o + 1, 1 - half)
            lhs = jnp.concatenate([occ[a, c], occ[b, c]], axis=1)
            rhs = jnp.concatenate([virt[r, pl.ds(c * 128, 128), :] for r in (a, b)], axis=0)
            total += jnp.dot(lhs, rhs, preferred_element_type=jnp.float32)
        acc[...] = total

    def z_arrived(c):
        z_copy(c).wait_recv()
        for i in range(3):
            xc_copy(c, i).start()

    def y_arrived(k):
        for way in range(2):
            y_copy(way, k).wait_recv()
            if k < 2:
                y_copy(way, k + 4).start()
            d_copy(way, k).start()
        if k + AHEAD < CH:
            z_copy(k + AHEAD).start()

    def d_arrived(k):
        for way in range(2):
            d_copy(way, k).wait_recv()

    def xc_arrived(c):
        for i in range(3):
            xc_copy(c, i).wait_recv()

    acc[...] = jnp.zeros_like(acc)
    y_arrived(0)
    y_arrived(1)
    hear(0)
    tell(1)
    y_arrived(2)
    z_arrived(0)
    y_arrived(3)
    z_arrived(1)
    y_arrived(4)
    z_arrived(2)
    y_arrived(5)
    hear(1)
    tell(2)
    z_arrived(3)
    own_copy().wait_recv()
    for i in range(3):
        x_copy(i).wait_recv()
    own_half(0)
    z_arrived(4)
    for k in range(4):
        d_arrived(k)
    own_half(1)
    own_half(3)
    z_arrived(5)
    d_arrived(4)
    d_arrived(5)
    own_half(2)
    hear(2)
    z_arrived(6)
    for pair in (0, 2):
        xc_arrived(pair)
        xc_arrived(pair + 1)
        for o in range(4):
            cross_half(o, pair, 2)
    z_arrived(7)
    xc_arrived(4)
    xc_arrived(5)
    for o in range(4):
        cross_half(o, 4, 2)
    for c in (6, 7):
        xc_arrived(c)
        last_cross(c)

    for j in range(2):
        flag = chi_mask[0, j].astype(jnp.float32)
        cols = pl.ds(j * 128, 128)
        chi[:, :, cols] = (acc[:, cols] * flag).astype(jnp.bfloat16).reshape(8, 16, 128)
    for distance in range(7, 0, -1):
        for to in (tau + distance, tau - distance):
            @pl.when(jnp.logical_and(to >= 0, to < 8))
            def _():
                t_copy(to, tau).start()

    regroup[tau] = chi[tau]
    for c in range(CH):
        z_copy(c).wait_send()
        for i in range(3):
            xc_copy(c, i).wait_send()
    for i in range(3):
        x_copy(i).wait_send()
    for k in range(6):
        for way in range(2):
            y_copy(way, k).wait_send()
            d_copy(way, k).wait_send()
    own_copy().wait_send()
    for o in range(1, 8):
        t_copy(lax.rem(tau + o, 8), tau).wait_send()
    own_slice = regroup[tau].astype(jnp.float32)
    totals = [own_slice * weights[k, tau] for k in range(8)]
    for o in range(1, 8):
        peer = lax.rem(tau + o, 8)
        t_copy(peer, peer).wait_recv()
        arrived = regroup[peer].astype(jnp.float32)
        totals = [total + arrived * weights[k, peer] for k, total in enumerate(totals)]
    for k in range(8):
        out_ref[k] = totals[k]


def shards(occupied, virtual_green, occ_mask, virt_mask, chi_mask, cosine_weights):
    dma = pltpu.SemaphoreType.DMA
    return pl.pallas_call(
        kernel,
        out_shape=pltpu.VMEM((8, 16, 256), jnp.float32),
        in_specs=[pl.BlockSpec(memory_space=pl.ANY)] * 6,
        out_specs=pl.BlockSpec(memory_space=pltpu.VMEM),
        scratch_shapes=[
            pltpu.VMEM((8, CH, 128, 128), jnp.bfloat16),
            pltpu.VMEM((8, 1024, 256), jnp.bfloat16),
            pltpu.VMEM((128, 256), jnp.float32),
            pltpu.VMEM((8, 16, 256), jnp.bfloat16),
            pltpu.VMEM((8, 16, 256), jnp.bfloat16),
            pltpu.SMEM((1, 8), jnp.int32),
            pltpu.SMEM((2, 8), jnp.int32),
            pltpu.SMEM((1, 2), jnp.int32),
            pltpu.SMEM((8, 8), jnp.float32),
            dma((CH + 5,)),
            dma((2, CH)),
            dma((2, 3)),
            dma((2, CH, 3)),
            dma((2, 2, 6)),
            dma((2, 2, 6)),
            dma((2,)),
            dma((2, 8)),
            pltpu.SemaphoreType.REGULAR((3,)),
        ],
        compiler_params=pltpu.CompilerParams(collective_id=0, has_side_effects=True),
        name="polarizability",
    )(occupied, virtual_green, occ_mask, virt_mask.T, chi_mask, cosine_weights)


def solution(mesh):
    placed = (
        P("tau", "row", "col"),
        P("tau", "row", "col"),
        P("row", "col"),
        P("row", "col"),
        P("row", "col"),
        P(),
    )
    return jax.shard_map(
        shards,
        mesh=mesh,
        in_specs=placed,
        out_specs=P(None, ("row", "tau"), "col"),
        check_vma=False,
    )
```

```python
import functools

import jax
import jax.numpy as jnp
from jax import lax
from jax.experimental import pallas as pl
from jax.experimental.pallas import tpu as pltpu
from jax.sharding import PartitionSpec as P

MESH = pl.DeviceIdType.MESH
CH = 8
LEAD = (3, 3, 2, 3, 3, 2, 3, 3)
AHEAD = max(LEAD)
OFFS = (2, 1, 3)


def kernel(
    occ_hbm, virt_hbm, occ_mask_hbm, virt_mask_hbm, chi_mask_hbm, weights_hbm, out_ref,
    occ, virt, acc, chi, regroup, occ_mask, virt_mask, chi_mask, weights,
    load_sem, z_sem, x_sem, xc_sem, y_sem, d_sem, own_sem, t_sem, reach_sem,
):
    tau = lax.axis_index("tau")
    row = lax.axis_index("row")
    col = lax.axis_index("col")
    y, core = row // 2, lax.rem(row, 2)
    x, half = col // 2, lax.rem(col, 2)
    mine = col
    cross = x * 2 + 1 - half

    def x_peer(o):
        return (tau, row, lax.rem(x + o, 4) * 2 + half)

    def y_peer(o):
        return (tau, lax.rem(y + o, 4) * 2 + core, col)

    partner = (tau, y * 2 + 1 - core, col)
    across = (tau, row, cross)

    barrier = pltpu.get_barrier_semaphore()
    for peer in [x_peer(o) for o in OFFS] + [y_peer(1), y_peer(3), partner, across]:
        pl.semaphore_signal(barrier, inc=1, device_id=peer, device_id_type=MESH)

    @pl.when(tau < 7)
    def _():
        pl.semaphore_signal(barrier, inc=1, device_id=(tau + 1, row, col), device_id_type=MESH)

    @pl.when(tau > 0)
    def _():
        pl.semaphore_signal(barrier, inc=1, device_id=(tau - 1, row, col), device_id_type=MESH)

    loads = [
        pltpu.make_async_copy(
            occ_hbm.at[0, :, pl.ds(c * 128, 128)], occ.at[mine, c], load_sem.at[c]
        )
        for c in range(CH)
    ]
    loads.append(pltpu.make_async_copy(virt_hbm.at[0], virt.at[row], load_sem.at[CH]))
    small = [
        pltpu.make_async_copy(src, dst, load_sem.at[CH + 1 + i])
        for i, (src, dst) in enumerate(
            [
                (occ_mask_hbm, occ_mask),
                (virt_mask_hbm, virt_mask),
                (chi_mask_hbm, chi_mask),
                (weights_hbm, weights),
            ]
        )
    ]
    small[0].start()
    for load in loads:
        load.start()
    for load in small[1:]:
        load.start()

    def masked(c):
        loads[c].wait()
        flag = occ_mask[0, c].astype(jnp.float32)
        occ[mine, c] = (occ[mine, c].astype(jnp.float32) * flag).astype(jnp.bfloat16)

    small[0].wait()
    for c in range(AHEAD):
        masked(c)
    ends = jnp.where(tau == 0, 1, 0) + jnp.where(tau == 7, 1, 0)
    pl.semaphore_wait(barrier, 9 - ends)

    def remote(src, dst, sems, at, peer):
        return pltpu.make_async_remote_copy(
            src_ref=src, dst_ref=dst, send_sem=sems.at[(0, *at)], recv_sem=sems.at[(1, *at)],
            device_id=peer, device_id_type=MESH,
        )

    def z_copy(c):
        return remote(occ.at[mine, c], occ.at[mine, c], z_sem, (c,), across)

    def x_copy(i):
        return remote(occ.at[mine], occ.at[mine], x_sem, (i,), x_peer(OFFS[i]))

    def xc_copy(c, i):
        return remote(occ.at[cross, c], occ.at[cross, c], xc_sem, (c, i), x_peer(OFFS[i]))

    def quarter(r, way, k):
        return virt.at[r, pl.ds(512 * ((way + k // 2) % 2) + 256 * (k % 2), 256)]

    def y_copy(way, k):
        r = row if k < 4 else lax.rem(y + 3 - 2 * way, 4) * 2 + core
        part = quarter(r, way, k)
        return remote(part, part, y_sem, (way, k), y_peer(1 + 2 * way))

    def d_copy(way, k):
        r = lax.rem(y + (3 - 2 * way if k < 4 else 2), 4) * 2 + core
        part = quarter(r, way, k)
        return remote(part, part, d_sem, (way, k), partner)

    def own_copy():
        return remote(virt.at[row], virt.at[row], own_sem, (), partner)

    def t_copy(to, sender):
        return pltpu.make_async_remote_copy(
            src_ref=chi.at[to], dst_ref=regroup.at[tau],
            send_sem=t_sem.at[0, to], recv_sem=t_sem.at[1, sender],
            device_id=(to, row, col), device_id_type=MESH,
        )

    ahead = sum(jnp.where(tau == t, LEAD[t], 0) for t in range(8))

    def z_start(step):
        for count in sorted(set(LEAD)):
            first = 0 if step < 0 else count + step
            last = count if step < 0 else CH if step == 5 else count + step + 1
            if first < CH:
                @pl.when(ahead == count)
                def _():
                    for c in range(first, min(last, CH)):
                        z_copy(c).start()

    z_start(-1)
    for c in range(AHEAD, CH):
        masked(c)
    for i in range(3):
        x_copy(i).start()
    loads[CH].wait()
    small[1].wait()
    for i in range(8):
        for j in range(2):
            flag = virt_mask[j, i].astype(jnp.float32)
            block = virt[row, pl.ds(i * 128, 128), pl.ds(j * 128, 128)]
            virt[row, pl.ds(i * 128, 128), pl.ds(j * 128, 128)] = (
                block.astype(jnp.float32) * flag
            ).astype(jnp.bfloat16)

    for k in range(4):
        for way in range(2):
            y_copy(way, k).start()
    own_copy().start()
    small[2].wait()
    small[3].wait()

    def tell(k):
        for step in (-(2**k), 2**k):
            @pl.when(jnp.logical_and(tau + step >= 0, tau + step < 8))
            def _():
                pl.semaphore_signal(
                    reach_sem.at[k], inc=1, device_id=(tau + step, row, col), device_id_type=MESH
                )

    def hear(k):
        below, above = jnp.where(tau >= 2**k, 1, 0), jnp.where(tau < 8 - 2**k, 1, 0)
        pl.semaphore_wait(reach_sem.at[k], below + above)

    tell(0)

    def dot_chunks(kb, first, count):
        total = None
        for c in range(first, first + count, 2):
            lhs = jnp.concatenate([occ[kb, c], occ[kb, c + 1]], axis=1)
            rhs = virt[kb, pl.ds(c * 128, 256), :]
            part = jnp.dot(lhs, rhs, preferred_element_type=jnp.float32)
            total = part if total is None else total + part
        return total

    def block_of(o, h):
        return lax.rem(y + 4 - o, 4) * 2 + h

    def own_half(o):
        acc[...] += dot_chunks(block_of(o, half), 0, CH)

    def cross_half(o, first, count):
        acc[...] += dot_chunks(block_of(o, 1 - half), first, count)

    def last_cross(c):
        total = acc[...]
        for o in (0, 2):
            a, b = block_of(o, 1 - half), block_of(o + 1, 1 - half)
            lhs = jnp.concatenate([occ[a, c], occ[b, c]], axis=1)
            rhs = jnp.concatenate([virt[r, pl.ds(c * 128, 128), :] for r in (a, b)], axis=0)
            total += jnp.dot(lhs, rhs, preferred_element_type=jnp.float32)
        acc[...] = total

    def z_arrived(c):
        z_copy(c).wait_recv()
        for i in range(3):
            xc_copy(c, i).start()

    def y_arrived(k):
        for way in range(2):
            y_copy(way, k).wait_recv()
            if k < 2:
                y_copy(way, k + 4).start()
            d_copy(way, k).start()
        z_start(k)

    def d_arrived(k):
        for way in range(2):
            d_copy(way, k).wait_recv()

    def xc_arrived(c):
        for i in range(3):
            xc_copy(c, i).wait_recv()

    acc[...] = jnp.zeros_like(acc)
    y_arrived(0)
    y_arrived(1)
    hear(0)
    tell(1)
    y_arrived(2)
    z_arrived(0)
    y_arrived(3)
    z_arrived(1)
    y_arrived(4)
    z_arrived(2)
    y_arrived(5)
    hear(1)
    tell(2)
    z_arrived(3)
    own_copy().wait_recv()
    for i in range(3):
        x_copy(i).wait_recv()
    own_half(0)
    z_arrived(4)
    for k in range(4):
        d_arrived(k)
    own_half(1)
    own_half(3)
    z_arrived(5)
    d_arrived(4)
    d_arrived(5)
    own_half(2)
    hear(2)
    z_arrived(6)
    for pair in (0, 2):
        xc_arrived(pair)
        xc_arrived(pair + 1)
        for o in range(4):
            cross_half(o, pair, 2)
    z_arrived(7)
    xc_arrived(4)
    xc_arrived(5)
    for o in range(4):
        cross_half(o, 4, 2)
    for c in (6, 7):
        xc_arrived(c)
        last_cross(c)

    for j in range(2):
        flag = chi_mask[0, j].astype(jnp.float32)
        cols = pl.ds(j * 128, 128)
        chi[:, :, cols] = (acc[:, cols] * flag).astype(jnp.bfloat16).reshape(8, 16, 128)
    for distance in range(7, 0, -1):
        for to in (tau + distance, tau - distance):
            @pl.when(jnp.logical_and(to >= 0, to < 8))
            def _():
                t_copy(to, tau).start()

    regroup[tau] = chi[tau]
    for c in range(CH):
        z_copy(c).wait_send()
        for i in range(3):
            xc_copy(c, i).wait_send()
    for i in range(3):
        x_copy(i).wait_send()
    for k in range(6):
        for way in range(2):
            y_copy(way, k).wait_send()
            d_copy(way, k).wait_send()
    own_copy().wait_send()
    for o in range(1, 8):
        t_copy(lax.rem(tau + o, 8), tau).wait_send()
    own_slice = regroup[tau].astype(jnp.float32)
    totals = [own_slice * weights[k, tau] for k in range(8)]
    for o in range(1, 8):
        peer = lax.rem(tau + o, 8)
        t_copy(peer, peer).wait_recv()
        arrived = regroup[peer].astype(jnp.float32)
        totals = [total + arrived * weights[k, peer] for k, total in enumerate(totals)]
    for k in range(8):
        out_ref[k] = totals[k]


def shards(occupied, virtual_green, occ_mask, virt_mask, chi_mask, cosine_weights):
    dma = pltpu.SemaphoreType.DMA
    return pl.pallas_call(
        kernel,
        out_shape=pltpu.VMEM((8, 16, 256), jnp.float32),
        in_specs=[pl.BlockSpec(memory_space=pl.ANY)] * 6,
        out_specs=pl.BlockSpec(memory_space=pltpu.VMEM),
        scratch_shapes=[
            pltpu.VMEM((8, CH, 128, 128), jnp.bfloat16),
            pltpu.VMEM((8, 1024, 256), jnp.bfloat16),
            pltpu.VMEM((128, 256), jnp.float32),
            pltpu.VMEM((8, 16, 256), jnp.bfloat16),
            pltpu.VMEM((8, 16, 256), jnp.bfloat16),
            pltpu.SMEM((1, 8), jnp.int32),
            pltpu.SMEM((2, 8), jnp.int32),
            pltpu.SMEM((1, 2), jnp.int32),
            pltpu.SMEM((8, 8), jnp.float32),
            dma((CH + 5,)),
            dma((2, CH)),
            dma((2, 3)),
            dma((2, CH, 3)),
            dma((2, 2, 6)),
            dma((2, 2, 6)),
            dma((2,)),
            dma((2, 8)),
            pltpu.SemaphoreType.REGULAR((3,)),
        ],
        compiler_params=pltpu.CompilerParams(collective_id=0, has_side_effects=True),
        name="polarizability",
    )(occupied, virtual_green, occ_mask, virt_mask.T, chi_mask, cosine_weights)


def solution(mesh):
    placed = (
        P("tau", "row", "col"),
        P("tau", "row", "col"),
        P("row", "col"),
        P("row", "col"),
        P("row", "col"),
        P(),
    )
    return jax.shard_map(
        shards,
        mesh=mesh,
        in_specs=placed,
        out_specs=P(None, ("row", "tau"), "col"),
        check_vma=False,
    )
```

```python
import functools

import jax
import jax.numpy as jnp
from jax import lax
from jax.experimental import pallas as pl
from jax.experimental.pallas import tpu as pltpu
from jax.sharding import PartitionSpec as P

MESH = pl.DeviceIdType.MESH
CH = 8
LEAD = (3, 3, 2, 2, 2, 2, 3, 3)
AHEAD = max(LEAD)
OFFS = (2, 1, 3)


def kernel(
    occ_hbm, virt_hbm, occ_mask_hbm, virt_mask_hbm, chi_mask_hbm, weights_hbm, out_ref,
    occ, virt, acc, chi, regroup, occ_mask, virt_mask, chi_mask, weights,
    load_sem, z_sem, x_sem, xc_sem, y_sem, d_sem, own_sem, t_sem, reach_sem,
):
    tau = lax.axis_index("tau")
    row = lax.axis_index("row")
    col = lax.axis_index("col")
    y, core = row // 2, lax.rem(row, 2)
    x, half = col // 2, lax.rem(col, 2)
    mine = col
    cross = x * 2 + 1 - half

    def x_peer(o):
        return (tau, row, lax.rem(x + o, 4) * 2 + half)

    def y_peer(o):
        return (tau, lax.rem(y + o, 4) * 2 + core, col)

    partner = (tau, y * 2 + 1 - core, col)
    across = (tau, row, cross)

    barrier = pltpu.get_barrier_semaphore()
    for peer in [x_peer(o) for o in OFFS] + [y_peer(1), y_peer(3), partner, across]:
        pl.semaphore_signal(barrier, inc=1, device_id=peer, device_id_type=MESH)

    @pl.when(tau < 7)
    def _():
        pl.semaphore_signal(barrier, inc=1, device_id=(tau + 1, row, col), device_id_type=MESH)

    @pl.when(tau > 0)
    def _():
        pl.semaphore_signal(barrier, inc=1, device_id=(tau - 1, row, col), device_id_type=MESH)

    loads = [
        pltpu.make_async_copy(
            occ_hbm.at[0, :, pl.ds(c * 128, 128)], occ.at[mine, c], load_sem.at[c]
        )
        for c in range(CH)
    ]
    loads.append(pltpu.make_async_copy(virt_hbm.at[0], virt.at[row], load_sem.at[CH]))
    small = [
        pltpu.make_async_copy(src, dst, load_sem.at[CH + 1 + i])
        for i, (src, dst) in enumerate(
            [
                (occ_mask_hbm, occ_mask),
                (virt_mask_hbm, virt_mask),
                (chi_mask_hbm, chi_mask),
                (weights_hbm, weights),
            ]
        )
    ]
    small[0].start()
    for load in loads:
        load.start()
    for load in small[1:]:
        load.start()

    def masked(c):
        loads[c].wait()
        flag = occ_mask[0, c].astype(jnp.float32)
        occ[mine, c] = (occ[mine, c].astype(jnp.float32) * flag).astype(jnp.bfloat16)

    small[0].wait()
    for c in range(AHEAD):
        masked(c)
    ends = jnp.where(tau == 0, 1, 0) + jnp.where(tau == 7, 1, 0)
    pl.semaphore_wait(barrier, 9 - ends)

    def remote(src, dst, sems, at, peer):
        return pltpu.make_async_remote_copy(
            src_ref=src, dst_ref=dst, send_sem=sems.at[(0, *at)], recv_sem=sems.at[(1, *at)],
            device_id=peer, device_id_type=MESH,
        )

    def z_copy(c):
        return remote(occ.at[mine, c], occ.at[mine, c], z_sem, (c,), across)

    def x_copy(i):
        return remote(occ.at[mine], occ.at[mine], x_sem, (i,), x_peer(OFFS[i]))

    def xc_copy(c, i):
        return remote(occ.at[cross, c], occ.at[cross, c], xc_sem, (c, i), x_peer(OFFS[i]))

    def quarter(r, way, k):
        return virt.at[r, pl.ds(512 * ((way + k // 2) % 2) + 256 * (k % 2), 256)]

    def y_copy(way, k):
        r = row if k < 4 else lax.rem(y + 3 - 2 * way, 4) * 2 + core
        part = quarter(r, way, k)
        return remote(part, part, y_sem, (way, k), y_peer(1 + 2 * way))

    def d_copy(way, k):
        r = lax.rem(y + (3 - 2 * way if k < 4 else 2), 4) * 2 + core
        part = quarter(r, way, k)
        return remote(part, part, d_sem, (way, k), partner)

    def own_copy():
        return remote(virt.at[row], virt.at[row], own_sem, (), partner)

    def t_copy(to, sender):
        return pltpu.make_async_remote_copy(
            src_ref=chi.at[to], dst_ref=regroup.at[tau],
            send_sem=t_sem.at[0, to], recv_sem=t_sem.at[1, sender],
            device_id=(to, row, col), device_id_type=MESH,
        )

    ahead = sum(jnp.where(tau == t, LEAD[t], 0) for t in range(8))

    def z_start(step):
        for count in sorted(set(LEAD)):
            first = 0 if step < 0 else count + step
            last = count if step < 0 else CH if step == 5 else count + step + 1
            if first < CH:
                @pl.when(ahead == count)
                def _():
                    for c in range(first, min(last, CH)):
                        z_copy(c).start()

    z_start(-1)
    for c in range(AHEAD, CH):
        masked(c)
    for i in range(3):
        x_copy(i).start()
    loads[CH].wait()
    small[1].wait()
    for i in range(8):
        for j in range(2):
            flag = virt_mask[j, i].astype(jnp.float32)
            block = virt[row, pl.ds(i * 128, 128), pl.ds(j * 128, 128)]
            virt[row, pl.ds(i * 128, 128), pl.ds(j * 128, 128)] = (
                block.astype(jnp.float32) * flag
            ).astype(jnp.bfloat16)

    for k in range(4):
        for way in range(2):
            y_copy(way, k).start()
    own_copy().start()
    small[2].wait()
    small[3].wait()

    def tell(k):
        for step in (-(2**k), 2**k):
            @pl.when(jnp.logical_and(tau + step >= 0, tau + step < 8))
            def _():
                pl.semaphore_signal(
                    reach_sem.at[k], inc=1, device_id=(tau + step, row, col), device_id_type=MESH
                )

    def hear(k):
        below, above = jnp.where(tau >= 2**k, 1, 0), jnp.where(tau < 8 - 2**k, 1, 0)
        pl.semaphore_wait(reach_sem.at[k], below + above)

    tell(0)

    def dot_chunks(kb, first, count):
        total = None
        for c in range(first, first + count, 2):
            lhs = jnp.concatenate([occ[kb, c], occ[kb, c + 1]], axis=1)
            rhs = virt[kb, pl.ds(c * 128, 256), :]
            part = jnp.dot(lhs, rhs, preferred_element_type=jnp.float32)
            total = part if total is None else total + part
        return total

    def block_of(o, h):
        return lax.rem(y + 4 - o, 4) * 2 + h

    def own_half(o):
        acc[...] += dot_chunks(block_of(o, half), 0, CH)

    def cross_half(o, first, count):
        acc[...] += dot_chunks(block_of(o, 1 - half), first, count)

    def last_cross(c):
        total = acc[...]
        for o in (0, 2):
            a, b = block_of(o, 1 - half), block_of(o + 1, 1 - half)
            lhs = jnp.concatenate([occ[a, c], occ[b, c]], axis=1)
            rhs = jnp.concatenate([virt[r, pl.ds(c * 128, 128), :] for r in (a, b)], axis=0)
            total += jnp.dot(lhs, rhs, preferred_element_type=jnp.float32)
        acc[...] = total

    def z_arrived(c):
        z_copy(c).wait_recv()
        for i in range(3):
            xc_copy(c, i).start()

    def y_arrived(k):
        for way in range(2):
            y_copy(way, k).wait_recv()
            if k < 2:
                y_copy(way, k + 4).start()
            d_copy(way, k).start()
        z_start(k)

    def d_arrived(k):
        for way in range(2):
            d_copy(way, k).wait_recv()

    def xc_arrived(c):
        for i in range(3):
            xc_copy(c, i).wait_recv()

    acc[...] = jnp.zeros_like(acc)
    y_arrived(0)
    y_arrived(1)
    hear(0)
    tell(1)
    y_arrived(2)
    z_arrived(0)
    y_arrived(3)
    z_arrived(1)
    y_arrived(4)
    z_arrived(2)
    y_arrived(5)
    hear(1)
    tell(2)
    z_arrived(3)
    own_copy().wait_recv()
    for i in range(3):
        x_copy(i).wait_recv()
    own_half(0)
    z_arrived(4)
    for k in range(4):
        d_arrived(k)
    own_half(1)
    own_half(3)
    z_arrived(5)
    d_arrived(4)
    d_arrived(5)
    own_half(2)
    hear(2)
    z_arrived(6)
    for pair in (0, 2):
        xc_arrived(pair)
        xc_arrived(pair + 1)
        for o in range(4):
            cross_half(o, pair, 2)
    z_arrived(7)
    xc_arrived(4)
    xc_arrived(5)
    for o in range(4):
        cross_half(o, 4, 2)
    for c in (6, 7):
        xc_arrived(c)
        last_cross(c)

    for j in range(2):
        flag = chi_mask[0, j].astype(jnp.float32)
        cols = pl.ds(j * 128, 128)
        chi[:, :, cols] = (acc[:, cols] * flag).astype(jnp.bfloat16).reshape(8, 16, 128)
    for distance in range(7, 0, -1):
        for to in (tau + distance, tau - distance):
            @pl.when(jnp.logical_and(to >= 0, to < 8))
            def _():
                t_copy(to, tau).start()

    regroup[tau] = chi[tau]
    for c in range(CH):
        z_copy(c).wait_send()
        for i in range(3):
            xc_copy(c, i).wait_send()
    for i in range(3):
        x_copy(i).wait_send()
    for k in range(6):
        for way in range(2):
            y_copy(way, k).wait_send()
            d_copy(way, k).wait_send()
    own_copy().wait_send()
    for o in range(1, 8):
        t_copy(lax.rem(tau + o, 8), tau).wait_send()
    own_slice = regroup[tau].astype(jnp.float32)
    totals = [own_slice * weights[k, tau] for k in range(8)]
    for o in range(1, 8):
        peer = lax.rem(tau + o, 8)
        t_copy(peer, peer).wait_recv()
        arrived = regroup[peer].astype(jnp.float32)
        totals = [total + arrived * weights[k, peer] for k, total in enumerate(totals)]
    for k in range(8):
        out_ref[k] = totals[k]


def shards(occupied, virtual_green, occ_mask, virt_mask, chi_mask, cosine_weights):
    dma = pltpu.SemaphoreType.DMA
    return pl.pallas_call(
        kernel,
        out_shape=pltpu.VMEM((8, 16, 256), jnp.float32),
        in_specs=[pl.BlockSpec(memory_space=pl.ANY)] * 6,
        out_specs=pl.BlockSpec(memory_space=pltpu.VMEM),
        scratch_shapes=[
            pltpu.VMEM((8, CH, 128, 128), jnp.bfloat16),
            pltpu.VMEM((8, 1024, 256), jnp.bfloat16),
            pltpu.VMEM((128, 256), jnp.float32),
            pltpu.VMEM((8, 16, 256), jnp.bfloat16),
            pltpu.VMEM((8, 16, 256), jnp.bfloat16),
            pltpu.SMEM((1, 8), jnp.int32),
            pltpu.SMEM((2, 8), jnp.int32),
            pltpu.SMEM((1, 2), jnp.int32),
            pltpu.SMEM((8, 8), jnp.float32),
            dma((CH + 5,)),
            dma((2, CH)),
            dma((2, 3)),
            dma((2, CH, 3)),
            dma((2, 2, 6)),
            dma((2, 2, 6)),
            dma((2,)),
            dma((2, 8)),
            pltpu.SemaphoreType.REGULAR((3,)),
        ],
        compiler_params=pltpu.CompilerParams(collective_id=0, has_side_effects=True),
        name="polarizability",
    )(occupied, virtual_green, occ_mask, virt_mask.T, chi_mask, cosine_weights)


def solution(mesh):
    placed = (
        P("tau", "row", "col"),
        P("tau", "row", "col"),
        P("row", "col"),
        P("row", "col"),
        P("row", "col"),
        P(),
    )
    return jax.shard_map(
        shards,
        mesh=mesh,
        in_specs=placed,
        out_specs=P(None, ("row", "tau"), "col"),
        check_vma=False,
    )
```
